256 devices in a mesh: sample: 4 (over y, x), gz: 64 (over z, core).
Axes of the slice: x: 2, y: 2, z: 32, core: 2. Of those that a mesh axis runs over, the one named last changes fastest.
The devices are a block of a 4x8x32 slice.
Arguments:
- spin_field: float32 [128, 96, 3, 1024], P('gz', 'sample'), parts along dimension 1, may hold values from -1 to 1, as said below
- couplings: int32 [128, 12, 1024], P('gz', 'sample'), parts along dimension 1, may hold values from 0 to 1
- parity_order: int32 [12], P('sample'), parts along dimension 0, may hold values from 0 to 1
- accept: int32 [92], P('sample'), parts along dimension 0, may hold values from 0 to 1
Outputs:
- new_spins: float32 [128, 96, 3, 1024], P('gz', 'sample'), parts along dimension 1
- energies: float32 [96], P('sample'), parts along dimension 0
The draws below stay inside these ranges and needn't reach their ends.
There are 4 independent parts, one for each index of `sample`. The reference program is written for one: setup_inputs(seed, part) draws one part's arguments, and reference() takes and returns one part's arrays. A program takes and returns all parts, laid end to end along the dimension named above; each array names one. Nothing has to cross between parts.
Inputs may be any that keep to these rules, and one draw needn't show every extreme that they name: `spin_field`: every site's spin has unit length.
All inputs are finite; a program needn't handle non-finite values.
Results may differ from the reference program's by a relative error of at most 0.00018.
Values sent between devices are 32-bit elements; how exact they have to be, the bound alone decides.
A program may use at most 64 MiB of HBM per device.

```python
import math
import jax
import jax.numpy as jnp
from jax import lax

NX = 32
NY = 32
R = 24
SWEEPS = 3
NZ = 128
PLANE = 1024


def draw_spin_field(key, part):
    values = jax.random.normal(key, (NZ, R, 3, NX * NY), jnp.float32)
    return values / jnp.sqrt(jnp.sum(values * values, axis=2, keepdims=True) + 1e-12)


def place_ends(array, rng, low, high):
    extent = array.shape
    index_at = [jax.random.randint(jax.random.fold_in(rng, axis), (), 0, extent[axis]) for axis in range(len(extent))]
    array = array.at[tuple(index_at)].set(low)
    longest = extent.index(max(extent))
    index_at[longest] = (index_at[longest] + 1) % extent[longest]
    return array.at[tuple(index_at)].set(high)


def setup_inputs(seed: int = 0, part: int = 0) -> dict:
    keys = jax.random.split(jax.random.key(seed), 5)
    part_keys = jax.random.split(jax.random.fold_in(keys[4], part), 5)
    return {
        "spin_field": draw_spin_field(jax.random.fold_in(jax.random.fold_in(keys[4], part), 71), part),
        "couplings": place_ends(jax.random.randint(part_keys[1], (NZ, 3, PLANE), 0, 2), jax.random.fold_in(part_keys[1], 1), 0, 1).astype(jnp.int32),
        "parity_order": jax.random.randint(part_keys[2], (SWEEPS,), 0, 2).astype(jnp.int32),
        "accept": place_ends(jax.random.randint(part_keys[3], (R - 1,), 0, 2), jax.random.fold_in(part_keys[3], 1), 0, 1).astype(jnp.int32),
    }


def plane_rolls(field, width_y):
    column = jnp.arange(field.shape[-1]) % width_y
    plus_x = jnp.roll(field, -width_y, axis=-1)
    minus_x = jnp.roll(field, width_y, axis=-1)
    plus_y = jnp.where(column == width_y - 1, jnp.roll(field, width_y - 1, axis=-1), jnp.roll(field, -1, axis=-1))
    minus_y = jnp.where(column == 0, jnp.roll(field, 1 - width_y, axis=-1), jnp.roll(field, 1, axis=-1))
    return (plus_x, minus_x, plus_y, minus_y)

def local_field(centre, lower_plane, upper_plane, bond_signs, bond_lower, width_y):
    plus_x, minus_x, plus_y, minus_y = plane_rolls(centre, width_y)
    shifted = plane_rolls(bond_signs, width_y)
    bond_x = bond_signs[:, 0][:, None, None, :]
    bond_y = bond_signs[:, 1][:, None, None, :]
    bond_z = bond_signs[:, 2][:, None, None, :]
    back_x = shifted[1][:, 0][:, None, None, :]
    back_y = shifted[3][:, 1][:, None, None, :]
    back_z = bond_lower[:, None, None, :]
    return bond_x * plus_x + back_x * minus_x + bond_y * plus_y + back_y * minus_y + bond_z * upper_plane + back_z * lower_plane

def overrelax(centre, local, selected):
    along = lax.optimization_barrier(jnp.sum(centre * local, axis=2, keepdims=True))
    strength = jnp.maximum(lax.optimization_barrier(jnp.sum(local * local, axis=2, keepdims=True)), 1.0)
    mirrored = 2.0 * along / strength * local - centre
    return jnp.where(selected[:, None, None, :], mirrored, centre)

def colour_map(planes, offset, plane_sites, width_y):
    height = jnp.arange(planes, dtype=jnp.int32)[:, None] + offset
    position = jnp.arange(plane_sites, dtype=jnp.int32)[None, :]
    return (position // width_y + position % width_y + height) % 2

def bond_terms(centre, upper_plane, bond_signs, width_y):
    plus_x, minus_x, plus_y, minus_y = plane_rolls(centre, width_y)
    bond_x = bond_signs[:, 0][:, None, None, :]
    bond_y = bond_signs[:, 1][:, None, None, :]
    bond_z = bond_signs[:, 2][:, None, None, :]
    return bond_x * plus_x + bond_y * plus_y + bond_z * upper_plane

def swap_order(accept):
    slots = accept.shape[0] + 1
    position = jnp.arange(slots, dtype=jnp.int32)
    accept_next = jnp.concatenate([accept, jnp.zeros((1,), jnp.int32)])
    accept_prev = jnp.concatenate([jnp.zeros((1,), jnp.int32), accept])
    slot_order = position
    for section_index in range(2):
        moves_up = ((position - section_index) % 2 == 0) & (accept_next == 1)
        moves_down = ((position - section_index) % 2 == 1) & (accept_prev == 1)
        source = position + moves_up.astype(jnp.int32) - moves_down.astype(jnp.int32)
        slot_order = slot_order[source]
    return slot_order

def reference(spin_field, couplings, parity_order, accept):
    bond_signs = (2 * couplings - 1).astype(jnp.float32)
    bond_lower = jnp.roll(bond_signs[:, 2], 1, axis=0)
    plane_sites = spin_field.shape[-1]
    colours = colour_map(NZ, jnp.int32(0), plane_sites, NY)
    spin_now = spin_field
    for sweep in range(SWEEPS):
        for half_step in range(2):
            target = (parity_order[sweep] + half_step) % 2
            local = local_field(spin_now, jnp.roll(spin_now, 1, axis=0), jnp.roll(spin_now, -1, axis=0), bond_signs, bond_lower, NY)
            spin_now = overrelax(spin_now, local, colours == target)
    bond_sum = bond_terms(spin_now, jnp.roll(spin_now, -1, axis=0), bond_signs, NY)
    raw = -lax.optimization_barrier(jnp.sum(spin_now * bond_sum, axis=(0, 2, 3))) / math.sqrt(NX * NY * NZ)
    slot_order = swap_order(accept)
    return (jnp.take(spin_now, slot_order, axis=1), raw[slot_order])
```

```python
import functools
import math

import jax
import jax.numpy as jnp
from jax import lax
from jax.experimental import pallas as pl
from jax.experimental.pallas import tpu as pltpu
from jax.sharding import PartitionSpec as P

NY = 32
SWEEPS = 3
STEPS = 2 * SWEEPS
LANES = 128
GROUP = 8
TILE = LANES // NY


def kernel(
    n,
    x_hbm,
    c_hbm,
    par_ref,
    acc_ref,
    out_hbm,
    energy_ref,
    xin,
    cpl,
    coef,
    jz,
    hist,
    part,
    sendbuf,
    recvbuf,
    outv,
    rows,
    gathered,
    apad,
    qs,
    in_sem,
    c_sem,
    out_sem,
    send_sem,
    recv_sem,
    know_sem,
    pair_sem,
    far_send,
    far_recv,
):
    _, comps, replicas, sites = x_hbm.shape
    groups = replicas // GROUP
    tiles = sites // LANES
    half = tiles // 2
    chips = n // 2
    me = lax.axis_index("gz")
    up, down = lax.rem(me + 1, n), lax.rem(me + n - 1, n)
    doublings = [1 << i for i in range(20) if (1 << i) <= n // 4]

    barrier = pltpu.get_barrier_semaphore()
    for neighbour in (down, up):
        pl.semaphore_signal(barrier, inc=1, device_id={"gz": neighbour})

    c_copy = pltpu.make_async_copy(c_hbm, cpl, c_sem)
    c_copy.start()
    x_copies = []
    for g in range(groups):
        window = pl.ds(g * GROUP, GROUP)
        x_copies.append(
            pltpu.make_async_copy(x_hbm.at[:, :, window, :], xin.at[:, :, window, :], in_sem.at[g])
        )
        x_copies[-1].start()

    lane = lax.broadcasted_iota(jnp.int32, (GROUP, LANES), 1)
    column = lane & (NY - 1)
    parity = (lax.shift_right_logical(lane, 5) + lane) & 1
    even = parity == 0

    def cut(k):
        return slice(k * LANES, (k + 1) * LANES)

    def rows_of(g):
        start = g * GROUP
        return pl.ds(start if isinstance(start, int) else pl.multiple_of(start, GROUP), GROUP)

    def shift_x(tiles_in):
        ahead = [pltpu.roll(t, LANES - NY, 1) for t in tiles_in]
        behind = [pltpu.roll(t, NY, 1) for t in tiles_in]
        count = len(tiles_in)
        plus = [jnp.where(lane < LANES - NY, ahead[k], ahead[(k + 1) % count]) for k in range(count)]
        minus = [jnp.where(lane >= NY, behind[k], behind[k - 1]) for k in range(count)]
        return plus, minus

    def plus_y(t):
        return jnp.where(column == NY - 1, pltpu.roll(t, NY - 1, 1), pltpu.roll(t, LANES - 1, 1))

    def minus_y(t):
        return jnp.where(column == 0, pltpu.roll(t, LANES - NY + 1, 1), pltpu.roll(t, 1, 1))

    def colour_of(step):
        return (par_ref[step // 2] + step % 2) % 2

    def changed(step):
        sweep = step // 2
        before = par_ref[jnp.maximum(sweep - 1, 0)]
        return (par_ref[sweep] + before) % 2

    def target_slot(step):
        return step + changed(step) * (1 - 2 * (step % 2))

    def near_slot(step):
        return step + 1 - changed(step) * (1 - step % 2)

    def lower_mask(colour):
        return ((parity + colour) & 1) == 0

    def halo_copy(step, g, way):
        return pltpu.make_async_remote_copy(
            src_ref=sendbuf.at[step, g, way],
            dst_ref=recvbuf.at[step, g, way],
            send_sem=send_sem.at[step, g, way],
            recv_sem=recv_sem.at[step, g, way],
            device_id={"gz": up if way == 0 else down},
        )

    def send_halo(step, g):
        mask = lower_mask(colour_of(step))
        slot = near_slot(step)
        for c in range(comps):
            for k in range(half):
                low = hist[slot, c, rows_of(g), cut(k)]
                high = hist[slot, c, rows_of(g), cut(k + half)]
                sendbuf[step, g, 0, c, :, cut(k)] = jnp.where(
                    mask, low * jz[1, :, cut(k)], pltpu.roll(high * jz[1, :, cut(k + half)], NY, 1)
                )
                sendbuf[step, g, 1, c, :, cut(k)] = jnp.where(mask, pltpu.roll(high, NY, 1), low)
        for way in range(2):
            halo_copy(step, g, way).start()

    def local_part(step, g):
        slot = near_slot(step)
        colour = colour_of(step)
        for c in range(comps):
            near = [hist[slot, c, rows_of(g), cut(k)] for k in range(tiles)]
            plus_x, minus_x = shift_x(near)
            for k in range(tiles):
                part[c, rows_of(g), cut(k)] = (
                    coef[colour, 0, :, cut(k)] * plus_x[k]
                    + coef[colour, 1, :, cut(k)] * minus_x[k]
                    + coef[colour, 2, :, cut(k)] * plus_y(near[k])
                    + coef[colour, 3, :, cut(k)] * minus_y(near[k])
                    + jz[0, :, cut(k)] * near[k]
                )

    def update(step, g, last=False):
        mask = lower_mask(colour_of(step))
        slot = target_slot(step)
        for way in range(2):
            halo_copy(step, g, way).wait_recv()
        energy = jnp.zeros((GROUP, LANES), jnp.float32)
        for k in range(half):
            outer = [[], []]
            for c in range(comps):
                from_below = recvbuf[step, g, 0, c, :, cut(k)]
                from_above = recvbuf[step, g, 1, c, :, cut(k)]
                outer[0].append(jnp.where(mask, from_below, from_above * jz[1, :, cut(k)]))
                other = pltpu.roll(jnp.where(mask, from_above, from_below), LANES - NY, 1)
                outer[1].append(jnp.where(mask, other, other * jz[1, :, cut(k + half)]))
            for side in range(2):
                where = cut(k + side * half)
                local = [part[c, rows_of(g), where] + outer[side][c] for c in range(comps)]
                spins = [hist[slot, c, rows_of(g), where] for c in range(comps)]
                along = sum(s * f for s, f in zip(spins, local))
                strength = jnp.maximum(sum(f * f for f in local), 1.0)
                factor = 2.0 * along / strength
                for c in range(comps):
                    new = factor * local[c] - spins[c]
                    hist[step + 2, c, rows_of(g), where] = new
                    if last:
                        energy += new * local[c]
        return energy

    c_copy.wait()
    bonds = []
    for d in range(3):
        bonds.append([])
        for z in range(2):
            signs = (2 * cpl[d, z : z + 1, :] - 1).astype(jnp.float32)
            signs = jnp.broadcast_to(signs, (GROUP, sites))
            bonds[d].append([signs[:, cut(k)] for k in range(tiles)])
    for z in range(2):
        for k in range(tiles):
            jz[z, :, cut(k)] = bonds[2][z][k]

    slot0_mask = lower_mask(par_ref[0])
    for g in range(groups):
        x_copies[g].wait()
        for c in range(comps):
            for k in range(tiles):
                lower = xin[0, c, rows_of(g), cut(k)]
                upper = xin[1, c, rows_of(g), cut(k)]
                hist[0, c, rows_of(g), cut(k)] = jnp.where(slot0_mask, lower, upper)
                hist[1, c, rows_of(g), cut(k)] = jnp.where(slot0_mask, upper, lower)
        if g == 0:
            pl.semaphore_wait(barrier, 2)
        send_halo(0, g)

    def greet(i):
        for way, there in enumerate((lax.rem(me + doublings[i], n), lax.rem(me + n - doublings[i], n))):
            pl.semaphore_signal(know_sem.at[i, way], inc=1, device_id={"gz": there})

    def heard(i):
        for way in range(2):
            pl.semaphore_wait(know_sem.at[i, way], 1)

    greet(0)

    shifted = [[shift_x(bonds[0][z])[1] for z in range(2)], [[minus_y(t) for t in bonds[1][z]] for z in range(2)]]
    for colour in range(2):
        for k in range(tiles):
            for j, signs in enumerate((bonds[0], shifted[0], bonds[1], shifted[1])):
                first, second = (signs[0][k], signs[1][k]) if colour == 0 else (signs[1][k], signs[0][k])
                coef[colour, j, :, cut(k)] = jnp.where(even, first, second)

    for g in range(groups):
        local_part(0, g)

    apad[0] = 0
    for k in range(replicas - 1):
        apad[k + 1] = acc_ref[k]
    apad[replicas] = 0
    accept_next = jnp.zeros((GROUP, LANES), jnp.int32)
    for k in range(replicas - 1):
        accept_next = jnp.where(lane == k, acc_ref[k], accept_next)
    accept_prev = pltpu.roll(accept_next, 1, 1)
    odd_slot = lane & 1
    first_source = lane + jnp.where(odd_slot == 0, accept_next, -accept_prev)
    order = jnp.where(
        odd_slot == 1,
        jnp.where(accept_next == 1, pltpu.roll(first_source, LANES - 1, 1), first_source),
        jnp.where(accept_prev == 1, pltpu.roll(first_source, 1, 1), first_source),
    )
    for t in range(replicas):
        middle = t + apad[t + 1] if t % 2 else t - apad[t]
        odd = middle % 2
        qs[t] = middle + (1 - odd) * apad[middle + 1] - odd * apad[middle]

    def one_step(step, carry):
        def one_group(g, inner):
            update(step, g)
            send_halo(step + 1, g)
            local_part(step + 1, g)
            return inner

        lax.fori_loop(0, groups, one_group, 0)
        for i in range(len(doublings)):
            @pl.when(step == i)
            def _():
                heard(i)
                if i + 1 < len(doublings):
                    greet(i + 1)
        return carry

    lax.fori_loop(0, STEPS - 1, one_step, 0)
    for i in range(STEPS - 1, len(doublings)):
        heard(i)
        if i + 1 < len(doublings):
            greet(i + 1)

    sublane = lax.broadcasted_iota(jnp.int32, (GROUP, LANES), 0)
    spread = jnp.zeros((GROUP, LANES), jnp.float32)
    for g in range(groups):
        energy = update(STEPS - 1, g, last=True)
        total = jnp.sum(energy, axis=1, keepdims=True)
        spread += jnp.where(order == sublane + g * GROUP, total, 0.0)
    rows[0] = jnp.sum(spread, axis=0, keepdims=True)

    chip = me // 2
    partner = me + 1 - 2 * (me % 2)
    pair = pltpu.make_async_remote_copy(
        src_ref=rows.at[0],
        dst_ref=rows.at[1],
        send_sem=pair_sem.at[0],
        recv_sem=pair_sem.at[1],
        device_id={"gz": partner},
    )
    pair.start()
    pair.wait_recv()
    rows[2] = rows[0] + rows[1]

    def far_copy(distance):
        return pltpu.make_async_remote_copy(
            src_ref=rows.at[2],
            dst_ref=gathered.at[chip],
            send_sem=far_send.at[distance],
            recv_sem=far_recv.at[chip],
            device_id={"gz": lax.rem(me + 2 * distance, n)},
        )

    far_first = sorted(range(1, chips), key=lambda d: -min(d, chips - d))
    for distance in far_first:
        far_copy(distance).start()
    gathered[chip] = rows[2]

    row_lane = lax.broadcasted_iota(jnp.int32, (1, sites), 1)
    row_parity = lax.shift_right_logical(row_lane, 5) + row_lane
    final_mask = ((row_parity + par_ref[SWEEPS - 1]) & 1) == 0

    def one_slot(t, carry):
        q = qs[t]
        for c in range(comps):
            first = hist[STEPS, c, pl.ds(q, 1), :]
            second = hist[STEPS + 1, c, pl.ds(q, 1), :]
            outv[0, c, pl.ds(t, 1), :] = jnp.where(final_mask, first, second)
            outv[1, c, pl.ds(t, 1), :] = jnp.where(final_mask, second, first)
        return carry

    lax.fori_loop(0, replicas, one_slot, 0)
    out_copy = pltpu.make_async_copy(outv, out_hbm, out_sem)
    out_copy.start()

    for distance in range(1, chips):
        source = lax.rem(chip + chips - distance, chips)
        pltpu.make_async_remote_copy(
            src_ref=rows.at[2],
            dst_ref=gathered.at[source],
            send_sem=far_send.at[distance],
            recv_sem=far_recv.at[source],
            device_id={"gz": lax.rem(me + 2 * distance, n)},
        ).wait_recv()
    scale = -1.0 / math.sqrt(sites * 2 * n)
    energy_ref[...] = jnp.sum(gathered[...], axis=0) * scale

    out_copy.wait()
    pair.wait_send()
    for distance in range(1, chips):
        far_copy(distance).wait_send()

    def drain(step, carry):
        def drain_group(g, inner):
            for way in range(2):
                halo_copy(step, g, way).wait_send()
            return inner

        return lax.fori_loop(0, groups, drain_group, carry)

    lax.fori_loop(0, STEPS, drain, 0)


def body(spin_field, couplings, parity_order, accept):
    planes, replicas, comps, sites = spin_field.shape
    n = lax.axis_size("gz")
    groups = replicas // GROUP
    chips = n // 2
    levels = max(1, sum(1 for i in range(20) if (1 << i) <= n // 4))
    dma = pltpu.SemaphoreType.DMA
    out, energy = pl.pallas_call(
        functools.partial(kernel, n),
        out_shape=(
            jax.ShapeDtypeStruct((planes, comps, replicas, sites), jnp.float32),
            jax.ShapeDtypeStruct((1, LANES), jnp.float32),
        ),
        in_specs=[
            pl.BlockSpec(memory_space=pl.ANY),
            pl.BlockSpec(memory_space=pl.ANY),
            pl.BlockSpec(memory_space=pltpu.SMEM),
            pl.BlockSpec(memory_space=pltpu.SMEM),
        ],
        out_specs=(pl.BlockSpec(memory_space=pl.ANY), pl.BlockSpec(memory_space=pltpu.VMEM)),
        scratch_shapes=[
            pltpu.VMEM((planes, comps, replicas, sites), jnp.float32),
            pltpu.VMEM((3, planes, sites), jnp.int32),
            pltpu.VMEM((2, 4, GROUP, sites), jnp.float32),
            pltpu.VMEM((2, GROUP, sites), jnp.float32),
            pltpu.VMEM((STEPS + 2, comps, replicas, sites), jnp.float32),
            pltpu.VMEM((comps, replicas, sites), jnp.float32),
            pltpu.VMEM((STEPS, groups, 2, comps, GROUP, sites // 2), jnp.float32),
            pltpu.VMEM((STEPS, groups, 2, comps, GROUP, sites // 2), jnp.float32),
            pltpu.VMEM((planes, comps, replicas, sites), jnp.float32),
            pltpu.VMEM((3, 1, LANES), jnp.float32),
            pltpu.VMEM((chips, 1, LANES), jnp.float32),
            pltpu.SMEM((replicas + 1,), jnp.int32),
            pltpu.SMEM((replicas,), jnp.int32),
            dma((groups,)),
            dma,
            dma,
            dma((STEPS, groups, 2)),
            dma((STEPS, groups, 2)),
            pltpu.SemaphoreType.REGULAR((levels, 2)),
            dma((2,)),
            dma((chips,)),
            dma((chips,)),
        ],
        compiler_params=pltpu.CompilerParams(collective_id=0, has_side_effects=True),
    )(spin_field.transpose(0, 2, 1, 3), couplings.transpose(1, 0, 2), parity_order, accept)
    return out.transpose(0, 2, 1, 3), energy[0, :replicas]


def solution(mesh):
    in_specs = (P("gz", "sample", None, None), P("gz", "sample", None), P("sample"), P("sample"))
    out_specs = (P("gz", "sample", None, None), P("sample"))
    return jax.shard_map(body, mesh=mesh, in_specs=in_specs, out_specs=out_specs, check_vma=False)
```

```python
import functools
import math

import jax
import jax.numpy as jnp
from jax import lax
from jax.experimental import pallas as pl
from jax.experimental.pallas import tpu as pltpu
from jax.sharding import PartitionSpec as P

NY = 32
SWEEPS = 3
STEPS = 2 * SWEEPS
LANES = 128
TILE = LANES // NY
GROUP = 8
UNITS = 4
NEWS_AT = ((0, 0), (0, 2), (1, 1), (2, 1))


def kernel(
    n,
    x_hbm,
    c_hbm,
    par_hbm,
    acc_hbm,
    out_ref,
    energy_ref,
    xin,
    cpl,
    coef,
    jz,
    hist,
    part,
    sendbuf,
    recvbuf,
    energy_row,
    gathered,
    par_ref,
    acc_ref,
    apad,
    qs,
    in_sem,
    c_sem,
    par_sem,
    acc_sem,
    send_sem,
    recv_sem,
    know_sem,
    far_sem,
):
    _, comps, replicas, sites = x_hbm.shape
    groups = replicas // GROUP
    tiles = sites // LANES
    half = tiles // 2
    pairs = half // UNITS
    me = lax.axis_index("gz")
    up, down = lax.rem(me + 1, n), lax.rem(me + n - 1, n)
    doublings = [1 << i for i in range(20) if (1 << i) <= n // 4]

    barrier = pltpu.get_barrier_semaphore()
    for neighbour in (down, up):
        pl.semaphore_signal(barrier, inc=1, device_id={"gz": neighbour})

    par_copy = pltpu.make_async_copy(par_hbm, par_ref, par_sem)
    par_copy.start()
    c_copy = pltpu.make_async_copy(c_hbm, cpl, c_sem)
    c_copy.start()
    x_copies = []
    for g in range(groups):
        window = pl.ds(g * GROUP, GROUP)
        x_copies.append(
            pltpu.make_async_copy(x_hbm.at[:, :, window, :], xin.at[:, :, window, :], in_sem.at[g])
        )
        x_copies[-1].start()
    acc_copy = pltpu.make_async_copy(acc_hbm, acc_ref, acc_sem)
    acc_copy.start()

    lane = lax.broadcasted_iota(jnp.int32, (GROUP, LANES), 1)
    column = lane & (NY - 1)
    low = lax.broadcasted_iota(jnp.int32, (GROUP, LANES), 0) < GROUP // 2
    plain_parity = (lax.shift_right_logical(lane, 5) + lane) & 1
    row = (lax.shift_right_logical(lane, 5) + jnp.where(low, 0, TILE - 1)) & (TILE - 1)
    parity = (row + lane) & 1
    last_row, first_row = row == TILE - 1, row == 0

    def into_frame(t):
        return jnp.where(low, t, pltpu.roll(t, NY, 1))

    def out_of_frame(t):
        return jnp.where(low, t, pltpu.roll(t, LANES - NY, 1))

    def swap_halves(t):
        return pltpu.roll(t, GROUP // 2, 0)

    def cut(k):
        return slice(k * LANES, (k + 1) * LANES)

    def shift_x(tiles_in):
        ahead = [pltpu.roll(t, LANES - NY, 1) for t in tiles_in]
        behind = [pltpu.roll(t, NY, 1) for t in tiles_in]
        count = len(tiles_in)
        plus = [jnp.where(last_row, ahead[(k + 1) % count], ahead[k]) for k in range(count)]
        minus = [jnp.where(first_row, behind[k - 1], behind[k]) for k in range(count)]
        return plus, minus

    def plus_y(t):
        return jnp.where(column == NY - 1, pltpu.roll(t, NY - 1, 1), pltpu.roll(t, LANES - 1, 1))

    def minus_y(t):
        return jnp.where(column == 0, pltpu.roll(t, LANES - NY + 1, 1), pltpu.roll(t, 1, 1))

    def minus_y_all(tiles_in):
        return [minus_y(t) for t in tiles_in]

    def colour_of(step):
        return (par_ref[step // 2] + step % 2) % 2

    def changed(step):
        sweep = step // 2
        before = par_ref[jnp.maximum(sweep - 1, 0)]
        return (par_ref[sweep] + before) % 2

    def target_slot(step):
        return step + changed(step) * (1 - 2 * (step % 2))

    def near_slot(step):
        return step + 1 - changed(step) * (1 - step % 2)

    def lower_mask(colour):
        return ((parity + colour) & 1) == 0

    def halo_copy(step, g, u, way):
        return pltpu.make_async_remote_copy(
            src_ref=sendbuf.at[step, g, u, way],
            dst_ref=recvbuf.at[step, g, u, way],
            send_sem=send_sem,
            recv_sem=recv_sem.at[step % 2, g, u],
            device_id={"gz": up if way == 0 else down},
        )

    def both_halos(step, g, u):
        return pltpu.make_async_remote_copy(
            src_ref=sendbuf.at[step, g, u],
            dst_ref=recvbuf.at[step, g, u],
            send_sem=send_sem,
            recv_sem=recv_sem.at[step % 2, g, u],
            device_id={"gz": up},
        )

    def fill_halo(step, g, u):
        mask = lower_mask(colour_of(step))
        slot = near_slot(step)
        for p in range(pairs):
            k = u * pairs + p
            for c in range(comps):
                to_above, to_below = [], []
                for tile in (k, k + half):
                    spins = hist[slot, c, g, tile]
                    swapped = swap_halves(spins)
                    to_above.append(jnp.where(mask, spins * jz[1, tile], swapped * jz[2, tile]))
                    to_below.append(jnp.where(mask, swapped, spins))
                sendbuf[step, g, u, 0, c, p] = jnp.where(low, *to_above)
                sendbuf[step, g, u, 1, c, p] = jnp.where(low, *to_below)

    def send_halo(step, g, u):
        for way in range(2):
            halo_copy(step, g, u, way).start()

    def local_part(step, g):
        slot = near_slot(step)
        colour = colour_of(step)
        for c in range(comps):
            near = [hist[slot, c, g, k] for k in range(tiles)]
            plus_x, minus_x = shift_x(near)
            for k in range(tiles):
                part[c, g, k] = (
                    coef[colour, 0, k] * plus_x[k]
                    + coef[colour, 1, k] * minus_x[k]
                    + coef[colour, 2, k] * plus_y(near[k])
                    + coef[colour, 3, k] * minus_y(near[k])
                    + jz[0, k] * near[k]
                )

    def update(step, g, u, energy=None):
        mask = lower_mask(colour_of(step))
        slot = target_slot(step)
        both_halos(step, g, u).wait_recv()
        for p in range(pairs):
            k = u * pairs + p
            outer = [[], []]
            for c in range(comps):
                below, above = recvbuf[step, g, u, 0, c, p], recvbuf[step, g, u, 1, c, p]
                below_swapped, above_swapped = swap_halves(below), swap_halves(above)
                outer[0].append(
                    jnp.where(
                        mask,
                        jnp.where(low, below, below_swapped),
                        jnp.where(low, above, above_swapped) * jz[1, k],
                    )
                )
                outer[1].append(
                    jnp.where(
                        mask,
                        jnp.where(low, below_swapped, below),
                        jnp.where(low, above_swapped, above) * jz[1, k + half],
                    )
                )
            for side in range(2):
                tile = k + side * half
                local = [part[c, g, tile] + outer[side][c] for c in range(comps)]
                spins = [hist[slot, c, g, tile] for c in range(comps)]
                along = sum(s * f for s, f in zip(spins, local))
                strength = jnp.maximum(sum(f * f for f in local), 1.0)
                factor = 2.0 * along / strength
                for c in range(comps):
                    new = factor * local[c] - spins[c]
                    hist[step + 2, c, g, tile] = new
                    if energy is not None:
                        energy += new * local[c]
        return energy

    def signs_of(d, z):
        signs = (2 * cpl[d, z : z + 1, :] - 1).astype(jnp.float32)
        signs = jnp.broadcast_to(signs, (GROUP, sites))
        return [signs[:, cut(k)] for k in range(tiles)]

    c_copy.wait()
    for z in range(2):
        for k, signs in enumerate(signs_of(2, z)):
            jz[z, k] = into_frame(signs)
            if z == 1:
                jz[2, k] = swap_halves(jz[1, k])
    par_copy.wait()
    first_mask = lower_mask(par_ref[0])
    for g in range(groups):
        x_copies[g].wait()
        window = slice(g * GROUP, (g + 1) * GROUP)
        for c in range(comps):
            for k in range(tiles):
                lower = into_frame(xin[0, c, window, cut(k)])
                upper = into_frame(xin[1, c, window, cut(k)])
                hist[0, c, g, k] = jnp.where(first_mask, lower, upper)
                hist[1, c, g, k] = jnp.where(first_mask, upper, lower)
        for u in range(UNITS):
            fill_halo(0, g, u)
            if g == 0 and u == 0:
                pl.semaphore_wait(barrier, 2)
            send_halo(0, g, u)

    def greet(i):
        for there in (lax.rem(me + doublings[i], n), lax.rem(me + n - doublings[i], n)):
            pl.semaphore_signal(know_sem.at[i], inc=1, device_id={"gz": there})

    def pass_on(i):
        pl.semaphore_wait(know_sem.at[i], 2)
        if i + 1 < len(doublings):
            greet(i + 1)

    greet(0)

    for j, (d, shift) in enumerate(((0, lambda t: t), (0, lambda t: shift_x(t)[1]), (1, lambda t: t), (1, minus_y_all))):
        lower, upper = (shift([into_frame(t) for t in signs_of(d, z)]) for z in range(2))
        for k in range(tiles):
            coef[0, j, k] = jnp.where(parity == 0, lower[k], upper[k])
            coef[1, j, k] = jnp.where(parity == 0, upper[k], lower[k])

    for g in range(groups):
        local_part(0, g)

    acc_copy.wait()
    apad[0] = 0
    for k in range(replicas - 1):
        apad[k + 1] = acc_ref[k]
    apad[replicas] = 0
    accept_next = jnp.zeros((GROUP, LANES), jnp.int32)
    for k in range(replicas - 1):
        accept_next = jnp.where(lane == k, acc_ref[k], accept_next)
    accept_prev = pltpu.roll(accept_next, 1, 1)
    odd_slot = lane & 1
    first_source = lane + jnp.where(odd_slot == 0, accept_next, -accept_prev)
    order = jnp.where(
        odd_slot == 1,
        jnp.where(accept_next == 1, pltpu.roll(first_source, LANES - 1, 1), first_source),
        jnp.where(accept_prev == 1, pltpu.roll(first_source, 1, 1), first_source),
    )
    for t in range(replicas):
        middle = t + apad[t + 1] if t % 2 else t - apad[t]
        odd = middle % 2
        qs[t] = middle + (1 - odd) * apad[middle + 1] - odd * apad[middle]

    def one_step(step, carry):
        for g in range(groups):
            for i, (at_step, at_group) in enumerate(NEWS_AT[: len(doublings)]):
                if g == at_group:
                    @pl.when(step == at_step)
                    def _():
                        pass_on(i)
            for u in range(UNITS):
                update(step, g, u)
                fill_halo(step + 1, g, u)
                send_halo(step + 1, g, u)
        for g in range(groups):
            local_part(step + 1, g)
        return carry

    lax.fori_loop(0, STEPS - 1, one_step, 0)

    sublane = lax.broadcasted_iota(jnp.int32, (GROUP, LANES), 0)
    spread = jnp.zeros((GROUP, LANES), jnp.float32)
    for g in range(groups):
        energy = jnp.zeros((GROUP, LANES), jnp.float32)
        for u in range(UNITS):
            energy = update(STEPS - 1, g, u, energy)
        total = jnp.sum(energy, axis=1, keepdims=True)
        spread += jnp.where(order == sublane + g * GROUP, total, 0.0)
    energy_row[...] = jnp.sum(spread, axis=0, keepdims=True)

    for i in range(len(NEWS_AT), len(doublings)):
        pass_on(i)

    def far_copy(distance):
        return pltpu.make_async_remote_copy(
            src_ref=energy_row,
            dst_ref=gathered.at[me],
            send_sem=far_sem.at[0],
            recv_sem=far_sem.at[1],
            device_id={"gz": lax.rem(me + distance, n)},
        )

    for distance in sorted(range(1, n), key=lambda d: abs(2 * d - n)):
        far_copy(distance).start()
    gathered[me] = energy_row[...]

    final_mask = ((plain_parity + par_ref[SWEEPS - 1]) & 1) == 0
    for g in range(groups):
        window = slice(g * GROUP, (g + 1) * GROUP)
        for c in range(comps):
            for k in range(tiles):
                first = out_of_frame(hist[STEPS, c, g, k])
                second = out_of_frame(hist[STEPS + 1, c, g, k])
                xin[0, c, window, cut(k)] = jnp.where(final_mask, first, second)
                xin[1, c, window, cut(k)] = jnp.where(final_mask, second, first)

    def one_slot(t, carry):
        for z in range(2):
            for c in range(comps):
                out_ref[z, c, pl.ds(t, 1), :] = xin[z, c, pl.ds(qs[t], 1), :]
        return carry

    lax.fori_loop(0, replicas, one_slot, 0)

    pltpu.make_async_remote_copy(
        src_ref=sendbuf,
        dst_ref=recvbuf,
        send_sem=send_sem,
        recv_sem=recv_sem.at[0, 0, 0],
        device_id={"gz": up},
    ).wait_send()
    others = gathered.at[pl.ds(0, n - 1)]
    all_far = pltpu.make_async_remote_copy(
        src_ref=others,
        dst_ref=others,
        send_sem=far_sem.at[0],
        recv_sem=far_sem.at[1],
        device_id={"gz": up},
    )
    all_far.wait_send()
    all_far.wait_recv()
    scale = -1.0 / math.sqrt(sites * 2 * n)
    energy_ref[...] = jnp.sum(gathered[...], axis=0) * scale


def body(spin_field, couplings, parity_order, accept):
    planes, replicas, comps, sites = spin_field.shape
    n = lax.axis_size("gz")
    groups = replicas // GROUP
    tiles = sites // LANES
    levels = max(1, sum(1 for i in range(20) if (1 << i) <= n // 4))
    dma = pltpu.SemaphoreType.DMA
    halo = (STEPS, groups, UNITS, 2)
    tile = (GROUP, LANES)
    anywhere = pl.BlockSpec(memory_space=pl.ANY)
    vmem = pl.BlockSpec(memory_space=pltpu.VMEM)
    out, energy = pl.pallas_call(
        functools.partial(kernel, n),
        out_shape=(
            pltpu.VMEM((planes, comps, replicas, sites), jnp.float32),
            pltpu.VMEM((1, LANES), jnp.float32),
        ),
        in_specs=[anywhere] * 4,
        out_specs=(vmem, vmem),
        scratch_shapes=[
            pltpu.VMEM((planes, comps, replicas, sites), jnp.float32),
            pltpu.VMEM((3, planes, sites), jnp.int32),
            pltpu.VMEM((2, 4, tiles, *tile), jnp.float32),
            pltpu.VMEM((3, tiles, *tile), jnp.float32),
            pltpu.VMEM((STEPS + 2, comps, groups, tiles, *tile), jnp.float32),
            pltpu.VMEM((comps, groups, tiles, *tile), jnp.float32),
            pltpu.VMEM((*halo, comps, tiles // 2 // UNITS, *tile), jnp.float32),
            pltpu.VMEM((*halo, comps, tiles // 2 // UNITS, *tile), jnp.float32),
            pltpu.VMEM((1, LANES), jnp.float32),
            pltpu.VMEM((n, 1, LANES), jnp.float32),
            pltpu.SMEM(parity_order.shape, jnp.int32),
            pltpu.SMEM(accept.shape, jnp.int32),
            pltpu.SMEM((replicas + 1,), jnp.int32),
            pltpu.SMEM((replicas,), jnp.int32),
            dma((groups,)),
            dma,
            dma,
            dma,
            dma,
            dma((2, groups, UNITS)),
            pltpu.SemaphoreType.REGULAR((levels,)),
            dma((2,)),
        ],
        compiler_params=pltpu.CompilerParams(collective_id=0, has_side_effects=True),
    )(spin_field.transpose(0, 2, 1, 3), couplings.transpose(1, 0, 2), parity_order, accept)
    return out.transpose(0, 2, 1, 3), energy[0, :replicas]


def solution(mesh):
    in_specs = (P("gz", "sample", None, None), P("gz", "sample", None), P("sample"), P("sample"))
    out_specs = (P("gz", "sample", None, None), P("sample"))
    return jax.shard_map(body, mesh=mesh, in_specs=in_specs, out_specs=out_specs, check_vma=False)
```
